32 devices in a mesh: groups: 2 (over y), vel: 4 (over z), space: 2 (over x), spec: 2 (over core).
Axes of the slice: x: 2, y: 2, z: 4, core: 2. Of those that a mesh axis runs over, the one named last changes fastest.
Arguments:
- distribution: float32 [2, 32, 64, 32768], P('spec', ('groups', 'space'), None, 'vel'), parts along dimension 1, may hold values from 0.25 to 4
- vel_order: int32 [32768], P('vel'), may hold values from 0 to 32767, each once
- species_mass: int32 [2], P('spec'), may hold values from 1 to 8
- wall_mask: int32 [32, 2], P(('groups', 'space')), parts along dimension 0, may hold values 0 or 1
- inflow_mask: int32 [32, 2], P(('groups', 'space')), parts along dimension 0, may hold values 0 or 1
Outputs:
- updated: float32 [2, 32, 64, 32768], P('spec', ('groups', 'space'), None, 'vel'), parts along dimension 1
The draws below stay inside these ranges and needn't reach their ends.
There are 2 independent parts, one for each index of `groups`. The reference program is written for one: setup_inputs(seed, part) draws one part's arguments, and reference() takes and returns one part's arrays. A program takes and returns all parts, laid end to end along the dimension named above; an argument that names none is the same for every part. Nothing has to cross between parts.
Inputs may be any that keep to these rules, and one draw needn't show every extreme that they name: `vel_order`: each number from 0 to 32767 appears once.
All inputs are finite; a program needn't handle non-finite values. No bound on the sum of `wall_mask` or of `inflow_mask` on one device may be relied on, other than what follows from the above.
Results may differ from the reference program's by a relative error of at most 0.0001.
Values sent between devices are 32-bit elements; how exact they have to be, the bound alone decides.
No kernel may reach another device: no remote copies, remote signals or barrier semaphores. Data moves between devices by JAX's collectives and lax.ppermute only.
A program may use at most 192 MiB of HBM per device.

```python
import math
import jax
import jax.numpy as jnp
from jax import lax

NV = 32
NY = 64
NVEL = 32768
NX = 16


def set_ends(array, rng, smallest, high):
    index_at = [jax.random.randint(jax.random.fold_in(rng, axis), (), 0, length) for axis, length in enumerate(array.shape)]
    main_axis = array.shape.index(max(array.shape))
    beside = index_at[:main_axis] + [(index_at[main_axis] + 1) % array.shape[main_axis]] + index_at[main_axis + 1:]
    return array.at[tuple(index_at)].set(smallest).at[tuple(beside)].set(high)


def levels(key, extent, split, low, top_value):
    level = 1.0
    for position, parts in split:
        heights = jax.random.uniform(jax.random.fold_in(jax.random.fold_in(key, 6), position), (parts,), jnp.float32, low / len(split), top_value / len(split))
        level = level * jnp.repeat(jnp.exp(heights), extent[position] // parts).reshape((-1,) + (1,) * (len(extent) - 1 - position))
    return level


def setup_inputs(seed: int = 0, part: int = 0) -> dict:
    keys = jax.random.split(jax.random.key(seed), 6)
    part_splits = jax.random.split(jax.random.fold_in(keys[5], part), 6)
    distribution = jnp.clip(jnp.exp(math.log(4.0) - 2.7725887 * jax.random.uniform(part_splits[0], (2, NX, NY, NVEL), jnp.float32) ** levels(part_splits[0], (2, NX, NY, NVEL), ((0, 2), (1, 2), (3, 4)), -0.2, 0.2)), 0.25, 4.0)
    vel_order = jax.random.permutation(keys[1], NVEL).astype(jnp.int32)
    species_mass = jax.random.randint(keys[2], (2,), 1, 9).astype(jnp.int32)
    wall_mask = set_ends((jax.random.randint(part_splits[3], (NX, 2), 0, 2) < 1).astype(jnp.int32), jax.random.fold_in(part_splits[3], 1), 0, 1)
    inflow_mask = set_ends((jax.random.randint(part_splits[4], (NX, 2), 0, 2) < 1).astype(jnp.int32), jax.random.fold_in(part_splits[4], 1), 0, 1)
    return {"distribution": distribution, "vel_order": vel_order, "species_mass": species_mass, "wall_mask": wall_mask, "inflow_mask": inflow_mask}


TIME_STEP = 0.1
RAREFACTION = 0.5
PORT_DENSITY = 1.0
HALF_RANGE = 4.5
PRECISE = lax.Precision.HIGHEST

def lattice(lattice_ids, molecule_weight):
    spacing = 2.0 * HALF_RANGE / (NV - 1) / jnp.sqrt(molecule_weight)
    centre = (NV - 1) / 2.0
    index_a = (lattice_ids // (NV * NV)).astype(jnp.float32)
    index_b = (lattice_ids // NV % NV).astype(jnp.float32)
    index_e = (lattice_ids % NV).astype(jnp.float32)
    return ((index_a - centre) * spacing, (index_b - centre) * spacing, (index_e - centre) * spacing, spacing)

def features(speed_x, speed_y, speed_z, molecule_weight):
    square = speed_x * speed_x + speed_y * speed_y + speed_z * speed_z
    unity = jnp.ones_like(speed_x)
    moment_rows = jnp.stack([unity, molecule_weight * unity, molecule_weight * speed_x, molecule_weight * speed_y, molecule_weight * speed_z, 0.5 * molecule_weight * square])
    shape_rows = jnp.stack([unity, speed_x, speed_y, speed_z, square])
    return (moment_rows, shape_rows, square)

def wall_law(square, spacing, molecule_weight):
    return jnp.exp(jnp.log(NVEL * spacing ** 3) + 1.5 * jnp.log(molecule_weight / (2.0 * jnp.pi)) - 0.5 * molecule_weight * square)

def wall_scale(molecule_weight):
    all_points = jnp.arange(NVEL, dtype=jnp.int32)
    speed_x, speed_y, speed_z, spacing = lattice(all_points, molecule_weight)
    square = speed_x * speed_x + speed_y * speed_y + speed_z * speed_z
    return jnp.sum(jnp.maximum(speed_y, 0.0) * wall_law(square, spacing, molecule_weight)) / NVEL

def mixture(first_moments, second_moments):
    blended_gas_sums_all = first_moments + second_moments
    count_per_volume = blended_gas_sums_all[0]
    component_weight_per_volume = blended_gas_sums_all[1]
    mean_drift_first = blended_gas_sums_all[2] / component_weight_per_volume
    mean_drift_second = blended_gas_sums_all[3] / component_weight_per_volume
    mean_drift_third = blended_gas_sums_all[4] / component_weight_per_volume
    motion_work_content = mean_drift_first * mean_drift_first + mean_drift_second * mean_drift_second + mean_drift_third * mean_drift_third
    cellwise_thermal_level = 2.0 / 3.0 * (blended_gas_sums_all[5] - 0.5 * component_weight_per_volume * motion_work_content) / count_per_volume
    return (mean_drift_first, mean_drift_second, mean_drift_third, cellwise_thermal_level, count_per_volume / RAREFACTION)

def coefficients(own_moments, blended_gas_mean, molecule_weight, spacing):
    mean_drift_first, mean_drift_second, mean_drift_third, cellwise_thermal_level, collision_pace = blended_gas_mean
    reciprocal_crowding = molecule_weight / cellwise_thermal_level
    motion_work_content = mean_drift_first * mean_drift_first + mean_drift_second * mean_drift_second + mean_drift_third * mean_drift_third
    leading = jnp.log(own_moments[0]) + jnp.log(NVEL * spacing ** 3) + 1.5 * jnp.log(reciprocal_crowding / (2.0 * jnp.pi)) - 0.5 * reciprocal_crowding * motion_work_content
    return jnp.stack([leading, reciprocal_crowding * mean_drift_first, reciprocal_crowding * mean_drift_second, reciprocal_crowding * mean_drift_third, -0.5 * reciprocal_crowding])

def collide(dist_rows, coeffs, collision_pace, shape_rows):
    exponent = lax.dot_general(coeffs, shape_rows, (((0,), (0,)), ((), ())), precision=PRECISE, preferred_element_type=jnp.float32)
    return dist_rows + TIME_STEP * collision_pace[:, None] * (jnp.exp(exponent) - dist_rows)

def stream(collided, left_cells, right_cells, ghost_low, ghost_high, speed_x, speed_y):
    below_cells = jnp.concatenate([ghost_low[:, None, :], collided[:, :-1, :]], axis=1)
    above_cells = jnp.concatenate([collided[:, 1:, :], ghost_high[:, None, :]], axis=1)
    plus_x = jnp.maximum(speed_x, 0.0)
    minus_x = jnp.minimum(speed_x, 0.0)
    plus_y = jnp.maximum(speed_y, 0.0)
    minus_y = jnp.minimum(speed_y, 0.0)
    change = plus_x * (collided - left_cells) + minus_x * (right_cells - collided) + plus_y * (collided - below_cells) + minus_y * (above_cells - collided)
    return collided - TIME_STEP * change

def reference(distribution, vel_order, species_mass, wall_mask, inflow_mask):
    masses = species_mass.astype(jnp.float32)
    cell_count = NX * NY
    moments = []
    incident = []
    for species in range(2):
        speed_x, speed_y, speed_z, spacing = lattice(vel_order, masses[species])
        moment_rows, shape_rows, square = features(speed_x, speed_y, speed_z, masses[species])
        flat_dist = distribution[species].reshape(cell_count, NVEL)
        moments.append(lax.dot_general(moment_rows, flat_dist, (((1,), (1,)), ((), ())), precision=PRECISE, preferred_element_type=jnp.float32) / NVEL)
        low_flux = jnp.dot(distribution[species][:, 0, :], jnp.maximum(-speed_y, 0.0), precision=PRECISE) / NVEL
        high_flux = jnp.dot(distribution[species][:, NY - 1, :], jnp.maximum(speed_y, 0.0), precision=PRECISE) / NVEL
        incident.append(jnp.stack([low_flux, high_flux], axis=1))
    blended_gas_mean = mixture(moments[0], moments[1])
    wall_weight = wall_mask.astype(jnp.float32)
    inflow_weight = inflow_mask.astype(jnp.float32)
    results = []
    for species in range(2):
        molecule_weight = masses[species]
        speed_x, speed_y, speed_z, spacing = lattice(vel_order, molecule_weight)
        moment_rows, shape_rows, square = features(speed_x, speed_y, speed_z, molecule_weight)
        flat_dist = distribution[species].reshape(cell_count, NVEL)
        coeffs = coefficients(moments[species], blended_gas_mean, molecule_weight, spacing)
        collided = collide(flat_dist, coeffs, blended_gas_mean[4], shape_rows).reshape(NX, NY, NVEL)
        emitted = wall_law(square, spacing, molecule_weight)
        factor = wall_weight * incident[species] / wall_scale(molecule_weight) + inflow_weight * PORT_DENSITY
        ghost_low = factor[:, 0:1] * emitted[None, :]
        ghost_high = factor[:, 1:2] * emitted[None, :]
        left_cells = jnp.roll(collided, 1, axis=0)
        right_cells = jnp.roll(collided, -1, axis=0)
        results.append(stream(collided, left_cells, right_cells, ghost_low, ghost_high, speed_x, speed_y))
    return jnp.stack(results)
```

```python
import math

import jax
import jax.numpy as jnp
import numpy as np
from jax import lax
from jax.experimental import pallas as pl
from jax.experimental.pallas import tpu as pltpu
from jax.sharding import PartitionSpec as P


NV = 32
NVEL = 32768

TIME_STEP = 0.1
RAREFACTION = 0.5
PORT_DENSITY = 1.0
HALF_RANGE = 4.5

LANES = 128
VMEM_LIMIT = 50 * 2**20
LOG2E = math.log2(math.e)
STEP = 2.0 * HALF_RANGE / (NV - 1)
ODD = 2.0 * np.arange(NV) - (NV - 1)
LAW_FRONT = NVEL * STEP**3 / (2.0 * math.pi) ** 1.5
LAW_RATE = STEP * STEP / 8.0
LAW_AXIS = np.exp(-LAW_RATE * ODD**2)
LAW_HALF = float(
    LAW_FRONT * 0.5 * STEP * np.sum(np.maximum(ODD, 0.0) * LAW_AXIS) * np.sum(LAW_AXIS) ** 2 / NVEL
)


def lattice_rows(ids):
    x = (2 * (ids // (NV * NV)) - (NV - 1)).astype(jnp.float32)
    y = (2 * (ids // NV % NV) - (NV - 1)).astype(jnp.float32)
    z = (2 * (ids % NV) - (NV - 1)).astype(jnp.float32)
    return x, y, z


def moments_kernel(mass_ref, ids_ref, dist_ref, rows_ref, part_ref, feat):
    vel = ids_ref.shape[1]
    cross = dist_ref.shape[1]
    tiles = vel // LANES
    groups = cross // 8
    mass = jnp.full((8, LANES), mass_ref[0], jnp.int32).astype(jnp.float32)
    half = 0.5 * STEP / jnp.sqrt(mass)

    @pl.when(pl.program_id(0) == 0)
    def _():
        def fill(t, carry):
            at = pl.ds(pl.multiple_of(t * LANES, LANES), LANES)
            ids = jnp.broadcast_to(ids_ref[:, at], (8, LANES))
            x, y, z = lattice_rows(ids)
            square = x * x + y * y + z * z
            high = square.astype(jnp.bfloat16).astype(jnp.float32)
            feat[0, :, at] = x
            feat[1, :, at] = y
            feat[2, :, at] = z
            feat[3, :, at] = square
            row = lax.broadcasted_iota(jnp.int32, (8, LANES), 0)
            out = jnp.where(row == 0, 1.0, x)
            out = jnp.where(row == 2, y, out)
            out = jnp.where(row == 3, z, out)
            out = jnp.where(row == 4, high, out)
            out = jnp.where(row == 5, square - high, out)
            out = jnp.where(row == 6, TIME_STEP * half * jnp.abs(x), out)
            out = jnp.where(row == 7, TIME_STEP * half * jnp.abs(y), out)
            rows_ref[:, at] = out
            return carry

        lax.fori_loop(0, tiles, fill, 0)

    def step(t, carry):
        sums, low, high = carry
        at = pl.ds(pl.multiple_of(t * LANES, LANES), LANES)
        x = feat[0, :, at]
        y = feat[1, :, at]
        z = feat[2, :, at]
        square = feat[3, :, at]
        new = []
        for g in range(groups):
            f = dist_ref[0, 8 * g : 8 * g + 8, at]
            n, mx, my, mz, e = sums[g]
            fy = f * y
            new.append((n + f, mx + f * x, my + fy, mz + f * z, e + f * square))
            if g == 0:
                low = low + jnp.maximum(-fy, 0.0)
            if g == groups - 1:
                high = high + jnp.maximum(fy, 0.0)
        return tuple(new), low, high

    zero = jnp.zeros((8, LANES), jnp.float32)
    sums, low, high = lax.fori_loop(
        0, tiles, step, (tuple((zero,) * 5 for _ in range(groups)), zero, zero)
    )
    scales = (
        jnp.full((8, LANES), 1.0 / NVEL, jnp.float32),
        mass * half / NVEL,
        mass * half / NVEL,
        mass * half / NVEL,
        0.5 * mass * half * half / NVEL,
        half / NVEL,
        mass / NVEL,
    )
    columns = [[sums[g][j] for g in range(groups)] for j in range(5)]
    columns.append([low] + [zero] * (groups - 2) + [high])
    columns.append(columns[0])
    row = lax.broadcasted_iota(jnp.int32, (8, LANES), 0)
    total = jnp.zeros((8, cross), jnp.float32)
    for j in range(7):
        picked = jnp.where(row == j, 1.0, 0.0)
        summed = lax.dot_general(
            picked,
            jnp.concatenate(columns[j], axis=0),
            (((1,), (1,)), ((), ())),
            precision=lax.Precision.HIGHEST,
            preferred_element_type=jnp.float32,
        )
        total = total + summed * scales[j][:, :cross]
    part_ref[0] = total


def moments(mass, ids, dist):
    rows, cross, vel = dist.shape
    return pl.pallas_call(
        moments_kernel,
        name="moments",
        grid=(rows,),
        in_specs=[
            pl.BlockSpec(memory_space=pltpu.SMEM),
            pl.BlockSpec((1, vel), lambda i: (0, 0)),
            pl.BlockSpec((1, cross, vel), lambda i: (i, 0, 0)),
        ],
        out_specs=[
            pl.BlockSpec((8, vel), lambda i: (0, 0)),
            pl.BlockSpec((1, 8, cross), lambda i: (i, 0, 0)),
        ],
        out_shape=[
            jax.ShapeDtypeStruct((8, vel), jnp.float32),
            jax.ShapeDtypeStruct((rows, 8, cross), jnp.float32),
        ],
        scratch_shapes=[pltpu.VMEM((4, 8, vel), jnp.float32)],
        compiler_params=pltpu.CompilerParams(
            dimension_semantics=("arbitrary",), vmem_limit_bytes=VMEM_LIMIT
        ),
    )(mass, ids, dist)


def coefficients_kernel(mass_ref, own_ref, other_ref, wall_ref, port_ref, coef_ref, fac_ref):
    rows, _, cross = own_ref.shape
    own = own_ref[...]
    total = own + other_ref[...]
    mass = jnp.full((rows, cross), mass_ref[0], jnp.int32).astype(jnp.float32)
    half = 0.5 * STEP / jnp.sqrt(mass)
    n = total[:, 0]
    r = total[:, 6]
    ux = total[:, 1] / r
    uy = total[:, 2] / r
    uz = total[:, 3] / r
    speed = ux * ux + uy * uy + uz * uz
    temperature = (2.0 / 3.0) * (total[:, 4] - 0.5 * r * speed) / n
    weight = TIME_STEP * (n / RAREFACTION)
    beta = mass / temperature
    leading = (
        jnp.log(own[:, 0])
        + math.log(LAW_FRONT)
        - 1.5 * jnp.log(temperature)
        - 0.5 * beta * speed
        + jnp.log(weight)
    )
    scale = LOG2E * beta * half
    square = -0.5 * scale * half
    coef_ref[:, 0] = LOG2E * leading
    coef_ref[:, 1] = scale * ux
    coef_ref[:, 2] = scale * uy
    coef_ref[:, 3] = scale * uz
    coef_ref[:, 4] = square
    coef_ref[:, 5] = square
    coef_ref[:, 6] = 1.0 - weight
    coef_ref[:, 7] = jnp.zeros_like(weight)
    wall = wall_ref[...].astype(jnp.float32)
    port = port_ref[...].astype(jnp.float32)
    incident = own[:, 5]
    share = jnp.sqrt(mass[:, :1]) / LAW_HALF
    for side, cell in ((0, 0), (1, cross - 1)):
        factor = (
            wall[:, side : side + 1] * incident[:, cell : cell + 1] * share
            + port[:, side : side + 1] * PORT_DENSITY
        )
        fac_ref[:, side] = jnp.broadcast_to(factor, (rows, LANES))


def coefficients(mass, own, other, wall_mask, inflow_mask):
    rows, _, cross = own.shape
    return pl.pallas_call(
        coefficients_kernel,
        name="coefficients",
        in_specs=[pl.BlockSpec(memory_space=pltpu.SMEM)]
        + [pl.BlockSpec(memory_space=pltpu.VMEM)] * 4,
        out_specs=[pl.BlockSpec(memory_space=pltpu.VMEM)] * 2,
        out_shape=[
            jax.ShapeDtypeStruct((rows, 8, cross), jnp.float32),
            jax.ShapeDtypeStruct((rows, 2, LANES), jnp.float32),
        ],
        compiler_params=pltpu.CompilerParams(vmem_limit_bytes=VMEM_LIMIT),
    )(mass, own, other, wall_mask, inflow_mask)


def split_columns(coef):
    row = lax.broadcasted_iota(jnp.int32, coef.shape, 0)
    rest = jnp.where(row < 6, coef, 0.0)
    pieces = []
    for _ in range(3):
        piece = rest.astype(jnp.bfloat16).astype(jnp.float32)
        pieces.append(piece)
        rest = rest - piece
    pieces.append(jnp.zeros_like(coef))
    return jnp.concatenate(pieces, axis=0).T.astype(jnp.bfloat16)


def split_rows(rows):
    return jnp.concatenate([rows, rows, rows, jnp.zeros_like(rows)], axis=0).astype(jnp.bfloat16)


def keep_column(coef, width):
    return jnp.broadcast_to(coef.T[:, 6:7], (coef.shape[1], width))


def slab_kernel(coef_ref, fac_ref, rows_ref, dist_ref, out_ref, table, keep):
    slab, cross, width = dist_ref.shape

    @pl.when(pl.program_id(0) == 0)
    def _():
        for x in range(slab):
            table[x] = split_columns(coef_ref[x])
            keep[x] = keep_column(coef_ref[x], LANES)

    def step(t, carry):
        at = pl.ds(pl.multiple_of(t * LANES, LANES), LANES)
        rows = rows_ref[:, at]
        shape = split_rows(rows)
        plus_x = rows[1:2] > 0.0
        plus_y = rows[2:3] > 0.0
        ax = rows[6:7]
        ay = rows[7:8]
        stay = 1.0 - ax - ay
        emitted = LAW_FRONT * jnp.exp2(-(LAW_RATE * LOG2E) * (rows[4:5] + rows[5:6]))
        row = lax.broadcasted_iota(jnp.int32, (cross, LANES), 0)

        def collided(x):
            exponent = jnp.dot(table[x], shape, preferred_element_type=jnp.float32)
            return dist_ref[x, :, at] * keep[x] + jnp.exp2(exponent)

        left = jnp.zeros((cross, LANES), jnp.float32)
        here = collided(0)
        for x in range(slab):
            right = collided(x + 1) if x + 1 < slab else jnp.zeros((cross, LANES), jnp.float32)
            below = jnp.where(row == 0, fac_ref[x, 0:1] * emitted, pltpu.roll(here, 1, axis=0))
            above = jnp.where(
                row == cross - 1, fac_ref[x, 1:2] * emitted, pltpu.roll(here, cross - 1, axis=0)
            )
            out_ref[x, :, at] = (
                stay * here
                + ax * jnp.where(plus_x, left, right)
                + ay * jnp.where(plus_y, below, above)
            )
            left, here = here, right
        return carry

    lax.fori_loop(0, width // LANES, step, 0)


def slab_update(coef, fac, rows, dist, width):
    slab, cross, vel = dist.shape
    return pl.pallas_call(
        slab_kernel,
        name="slab_update",
        grid=(vel // width,),
        in_specs=[
            pl.BlockSpec((slab, 8, cross), lambda k: (0, 0, 0)),
            pl.BlockSpec((slab, 2, LANES), lambda k: (0, 0, 0)),
            pl.BlockSpec((8, width), lambda k: (0, k)),
            pl.BlockSpec((slab, cross, width), lambda k: (0, 0, k)),
        ],
        out_specs=pl.BlockSpec((slab, cross, width), lambda k: (0, 0, k)),
        out_shape=jax.ShapeDtypeStruct((slab, cross, vel), jnp.float32),
        scratch_shapes=[
            pltpu.VMEM((slab, cross, 32), jnp.bfloat16),
            pltpu.VMEM((slab, cross, LANES), jnp.float32),
        ],
        compiler_params=pltpu.CompilerParams(
            dimension_semantics=("arbitrary",), vmem_limit_bytes=VMEM_LIMIT
        ),
    )(coef, fac, rows, dist)


def edge_kernel(left_ref, right_ref, rows_ref, halo_ref, in_ref, out_ref, gain):
    _, width = halo_ref.shape
    side = pl.program_id(1)

    @pl.when(side == 0)
    def _():
        table = jnp.concatenate(
            [split_columns(left_ref[...]), split_columns(right_ref[...])], axis=1
        )
        keep_left = keep_column(left_ref[...], LANES)
        keep_right = keep_column(right_ref[...], LANES)

        def step(t, carry):
            at = pl.ds(pl.multiple_of(t * LANES, LANES), LANES)
            rows = rows_ref[:, at]
            plus = rows[1:2] > 0.0
            shape = jnp.concatenate(
                [
                    split_rows(jnp.where(plus, rows, 0.0)),
                    split_rows(jnp.where(plus, 0.0, rows)),
                ],
                axis=0,
            )
            exponent = jnp.dot(table, shape, preferred_element_type=jnp.float32)
            value = rows[6:7] * (
                halo_ref[:, at] * jnp.where(plus, keep_left, keep_right) + jnp.exp2(exponent)
            )
            gain[:, at] = value
            out_ref[0, :, at] = in_ref[0, :, at] + jnp.where(plus, value, 0.0)
            return carry

        lax.fori_loop(0, width // LANES, step, 0)

    @pl.when(side == 1)
    def _():
        def step(t, carry):
            at = pl.ds(pl.multiple_of(t * LANES, LANES), LANES)
            plus = rows_ref[1:2, at] > 0.0
            out_ref[0, :, at] = in_ref[0, :, at] + jnp.where(plus, 0.0, gain[:, at])
            return carry

        lax.fori_loop(0, width // LANES, step, 0)


def edge_update(left, right, rows, halo, updated, start, width):
    slab, cross, _ = updated.shape
    first = start // width
    return pl.pallas_call(
        edge_kernel,
        name="edge_update",
        grid=(halo.shape[1] // width, 2),
        in_specs=[
            pl.BlockSpec((8, cross), lambda k, s: (0, 0)),
            pl.BlockSpec((8, cross), lambda k, s: (0, 0)),
            pl.BlockSpec((8, width), lambda k, s: (0, first + k)),
            pl.BlockSpec((cross, width), lambda k, s: (0, k)),
            pl.BlockSpec((1, cross, width), lambda k, s: (s * (slab - 1), 0, first + k)),
        ],
        out_specs=pl.BlockSpec((1, cross, width), lambda k, s: (s * (slab - 1), 0, first + k)),
        out_shape=jax.ShapeDtypeStruct(updated.shape, jnp.float32),
        scratch_shapes=[pltpu.VMEM((cross, width), jnp.float32)],
        input_output_aliases={4: 0},
        compiler_params=pltpu.CompilerParams(
            dimension_semantics=("arbitrary", "arbitrary"), vmem_limit_bytes=VMEM_LIMIT
        ),
    )(left, right, rows, halo, updated)


def select_kernel(ids_ref, tail_ref, head_ref, out_ref):
    plus = ids_ref[...] >= NV * NV * NV // 2
    out_ref[...] = jnp.where(plus, tail_ref[0], head_ref[0])


def select_edges(ids, dist, after, start, end, width):
    slab, cross, _ = dist.shape
    first = start // width
    gates = [] if after is None else [after]

    def kernel(*refs):
        select_kernel(*refs[len(gates) :])

    return pl.pallas_call(
        kernel,
        name="select_edges",
        grid=((end - start) // width,),
        in_specs=[pl.BlockSpec(memory_space=pl.ANY)] * len(gates)
        + [
            pl.BlockSpec((1, width), lambda k: (0, first + k)),
            pl.BlockSpec((1, cross, width), lambda k: (slab - 1, 0, first + k)),
            pl.BlockSpec((1, cross, width), lambda k: (0, 0, first + k)),
        ],
        out_specs=pl.BlockSpec((cross, width), lambda k: (0, k)),
        out_shape=jax.ShapeDtypeStruct((cross, end - start), jnp.float32),
        compiler_params=pltpu.CompilerParams(
            dimension_semantics=("arbitrary",), vmem_limit_bytes=VMEM_LIMIT
        ),
    )(*gates, ids, dist, dist)


def both_ways(tail, head, axis):
    count = lax.axis_size(axis)
    if count == 1:
        return tail, head
    return (
        lax.ppermute(tail, axis, [(i, (i + 1) % count) for i in range(count)]),
        lax.ppermute(head, axis, [((i + 1) % count, i) for i in range(count)]),
    )


def edge_cells(ids, dist, after, start, end, width, axis):
    count = lax.axis_size(axis)
    if count > 2:
        tail, head = dist[-1, :, start:end], dist[0, :, start:end]
        if after is not None:
            tail, head = lax.optimization_barrier((tail, head, after))[:2]
        from_left, from_right = both_ways(tail, head, axis)
        return jnp.where(ids[:, start:end] >= NV * NV * NV // 2, from_left, from_right)
    chosen = select_edges(ids, dist, after, start, end, width)
    if count == 2:
        chosen = lax.ppermute(chosen, axis, [(0, 1), (1, 0)])
    return chosen


def edge_coefficients(coef, axis):
    count = lax.axis_size(axis)
    if count == 2:
        pair = lax.ppermute(jnp.stack([coef[-1], coef[0]]), axis, [(0, 1), (1, 0)])
        return pair[0], pair[1]
    return both_ways(coef[-1], coef[0], axis)


def summed(part, axis):
    count = lax.axis_size(axis)
    if count & (count - 1):
        return lax.psum(part, axis)
    step = 1
    while step < count:
        part = part + lax.ppermute(part, axis, [(i, i ^ step) for i in range(count)])
        step *= 2
    return part


def chunk_ends(tiles):
    ends = sorted({max(1, tiles // 16), tiles // 2, tiles - max(1, tiles // 8), tiles})
    return [LANES * end for end in ends]


def body(distribution, vel_order, species_mass, wall_mask, inflow_mask):
    dist = distribution[0]
    _, _, vel = dist.shape
    ids = vel_order[None]
    ends = chunk_ends(vel // LANES)
    starts = [0] + ends[:-1]
    widths = [min(math.gcd(start, end - start) if start else end, 1024) for start, end in zip(starts, ends)]
    halos = []
    for start, end, width in zip(starts, ends, widths):
        if end <= vel // 2:
            halos.append(edge_cells(ids, dist, None, start, end, width, "space"))
    rows, part = moments(species_mass, ids, dist)
    own = summed(part, "vel")
    other = lax.ppermute(own, "spec", [(0, 1), (1, 0)])
    coef, fac = coefficients(species_mass, own, other, wall_mask, inflow_mask)
    left, right = edge_coefficients(coef, "space")
    for start, end, width in zip(starts, ends, widths):
        if end > vel // 2:
            halos.append(edge_cells(ids, dist, coef, start, end, width, "space"))
    updated = slab_update(coef, fac, rows, dist, min(vel, 512))
    for start, halo, width in zip(starts, halos, widths):
        updated = edge_update(left, right, rows, halo, updated, start, width)
    return updated[None]


def solution(mesh):
    in_specs = (
        P("spec", ("groups", "space"), None, "vel"),
        P("vel"),
        P("spec"),
        P(("groups", "space"), None),
        P(("groups", "space"), None),
    )
    out_specs = P("spec", ("groups", "space"), None, "vel")
    return jax.shard_map(body, mesh=mesh, in_specs=in_specs, out_specs=out_specs, check_vma=False)
```
